8 devices in a mesh: data: 1 (over z), tp: 8 (over y, x, core).
Axes of the slice: x: 2, y: 2, z: 1, core: 2. Of those that a mesh axis runs over, the one named last changes fastest.
Arguments:
- X: bfloat16 [2048, 4096], P(('data', 'tp'))
- gamma: float32 [4096], replicated
- W1: bfloat16 [4096, 14336], P(None, 'tp')
- W2: bfloat16 [14336, 4096], P('tp')
- dY: bfloat16 [2048, 4096], P(('data', 'tp'))
Outputs:
- output 1: bfloat16 [2048, 4096], P(('data', 'tp'))
- output 2: bfloat16 [2048, 4096], P(('data', 'tp'))
- output 3: float32 [4096, 14336], P('data', 'tp')
- output 4: float32 [14336, 4096], P(('data', 'tp'))
- output 5: float32 [4096], P('data')
All inputs are finite; a program needn't handle non-finite values.
Results may differ from the reference program's by a relative error of at most 0.001.
Values are sent between devices in bfloat16 or wider.
A program may use at most 1 GiB of HBM per device.

```python
import jax
import jax.numpy as jnp
from jax import lax

S = 2048
D = 4096
F = 14336
EPS = 1e-6


def setup_inputs(seed: int = 0, part: int = 0) -> dict:
    key = jax.random.key(seed)
    kg, k1, k2, kbase = jax.random.split(key, 4)
    kx, ky = jax.random.split(jax.random.fold_in(kbase, part))
    X = jax.random.normal(kx, (S, D), jnp.float32).astype(jnp.bfloat16)
    gamma = 1.0 + 0.2 * jax.random.normal(kg, (D,), jnp.float32)
    W1 = (jax.random.normal(k1, (D, F), jnp.float32) * D ** -0.5).astype(jnp.bfloat16)
    W2 = (jax.random.normal(k2, (F, D), jnp.float32) * (1.5 * F ** -0.5)).astype(jnp.bfloat16)
    dY = jax.random.normal(ky, (S, D), jnp.float32).astype(jnp.bfloat16)
    return {"X": X, "gamma": gamma, "W1": W1, "W2": W2, "dY": dY}


def _gelu(a):
    return jax.nn.gelu(a, approximate=True)


def reference(X, gamma, W1, W2, dY):
    x = X.astype(jnp.float32)
    mu = jnp.mean(x, axis=-1, keepdims=True)
    xc = x - mu
    var = jnp.mean(xc * xc, axis=-1, keepdims=True)
    rstd = lax.rsqrt(var + EPS)
    xhatv = xc * rstd
    Xn = (xhatv * gamma).astype(jnp.bfloat16)
    A = jnp.dot(Xn, W1, preferred_element_type=jnp.float32)
    H = _gelu(A).astype(jnp.bfloat16)
    Y = (x + jnp.dot(H, W2, preferred_element_type=jnp.float32)).astype(jnp.bfloat16)
    dW2 = jnp.dot(H.T, dY, preferred_element_type=jnp.float32)
    dH = jnp.dot(dY, W2.T, preferred_element_type=jnp.float32)
    dA = jax.vjp(_gelu, A)[1](dH)[0].astype(jnp.bfloat16)
    dW1 = jnp.dot(Xn.T, dA, preferred_element_type=jnp.float32)
    dXn = jnp.dot(dA, W1.T, preferred_element_type=jnp.float32)
    dgamma = jnp.sum(dXn * xhatv, axis=0)
    dxhat = dXn * gamma
    dx = rstd * (dxhat - jnp.mean(dxhat, axis=-1, keepdims=True) - xhatv * jnp.mean(dxhat * xhatv, axis=-1, keepdims=True))
    dX = (dY.astype(jnp.float32) + dx).astype(jnp.bfloat16)
    return (Y, dX, dW1, dW2, dgamma)
```

```python
import jax
import jax.numpy as jnp
from jax import lax
from jax.experimental import pallas as pl
from jax.experimental.pallas import tpu as pltpu
from jax.sharding import PartitionSpec as P


EPS = 1e-6


CORE, XN, YN, DIAG = 1, 2, 4, 6
NN = (((1,), (0,)), ((), ()))
NT = (((1,), (1,)), ((), ()))
ANY = pl.BlockSpec(memory_space=pl.ANY)


C1, C2 = 0.7978845608028654, 0.7978845608028654 * 0.044715


def _gelu(a):
    s = a * a
    q = 0.5 + 0.5 * jnp.tanh(a * (C1 + C2 * s))
    h = a * q
    return h, q + (h - h * q) * (2 * C1 + (6 * C2) * s)


def _ln(x):
    mu = jnp.mean(x, axis=-1, keepdims=True)
    xc = x - mu
    var = jnp.mean(xc * xc, axis=-1, keepdims=True)
    rstd = lax.rsqrt(var + EPS)
    return xc * rstd, rstd


def _tn(a, b):
    return lax.dot_general(a, b, (((0,), (0,)), ((), ())), preferred_element_type=jnp.float32)


def _dot(a, b, dims):
    return lax.dot_general(a, b, dims, preferred_element_type=jnp.float32)


def _swap(v, k):
    return lax.ppermute(v, "tp", [(i, i ^ k) for i in range(8)])


def _cost(m, k, n, extra=0):
    return pl.CostEstimate(flops=2 * m * k * n, bytes_accessed=2 * k * n + 2 * m * k + extra, transcendentals=0)


def _params():
    return pltpu.CompilerParams(dimension_semantics=("arbitrary",), vmem_limit_bytes=60 << 20)


def _fill(pieces, cat):
    if cat is None:
        return pieces[0][...]

    @pl.when(pl.program_id(0) == 0)
    def _():
        at = 0
        for p in pieces:
            cat[at:at + p.shape[0]] = p[...]
            at += p.shape[0]

    return cat[...]


def _up(pieces, weights, dims, slopes=None, after=(), tile=256):
    m, D = sum(p.shape[0] for p in pieces), pieces[0].shape[1]
    nt = dims == NT
    F = weights[0].shape[0 if nt else 1]
    nw, npc, ns = len(weights), len(pieces), len(slopes or ())

    def body(*refs):
        ps, ws, ss = refs[:npc], refs[npc:npc + nw], refs[npc + nw:npc + nw + ns]
        outs = refs[npc + nw + ns + len(after):]
        a = _fill(ps, refs[-1] if npc > 1 else None)
        for i in range(nw):
            r = _dot(a, ws[i][...], dims)
            if slopes:
                outs[i][...] = (ss[i][...] * r).astype(jnp.bfloat16)
            else:
                h, slope = _gelu(r)
                outs[2 * i][...] = h.astype(jnp.bfloat16)
                outs[2 * i + 1][...] = slope

    w_spec = pl.BlockSpec((tile, D), lambda j: (j, 0)) if nt else pl.BlockSpec((D, tile), lambda j: (0, j))
    o_spec = pl.BlockSpec((m, tile), lambda j: (0, j))
    types = [jnp.bfloat16] * nw if slopes else [jnp.bfloat16, jnp.float32] * nw
    return pl.pallas_call(
        body, grid=(F // tile,),
        in_specs=[pl.BlockSpec(p.shape, lambda j: (0, 0)) for p in pieces] + [w_spec] * nw
        + [o_spec] * ns + [ANY] * len(after),
        out_specs=[o_spec] * len(types),
        out_shape=[jax.ShapeDtypeStruct((m, F), t) for t in types],
        scratch_shapes=[pltpu.VMEM((m, D), jnp.bfloat16)] if npc > 1 else [],
        compiler_params=_params(), cost_estimate=_cost(m, D, F * nw),
        name="up_dA" if slopes else "up_A",
    )(*pieces, *weights, *(slopes or ()), *after)


def _down(parts, weights, dims, split=1, after=(), tile=512):
    F = parts[0][0].shape[1]
    m, nb = sum(p.shape[0] for p in parts[0]), len(parts[0])
    ms = [p.shape[0] // split for p in parts[0] for _ in range(split)]
    nt = dims == NT
    D = weights[0].shape[0 if nt else 1]
    n = len(parts)
    half, steps = D // 2, D // tile
    nin = n * nb

    def body(*refs):
        ws, outs = refs[nin:nin + n], refs[nin + n + len(after):]
        cats = outs[2 * len(ms):] or [None] * n
        r = None
        for i in range(n):
            d = _dot(_fill(refs[i * nb:(i + 1) * nb], cats[i]), ws[i][...], dims)
            r = d if r is None else r + d

        for h, on in enumerate((pl.program_id(0) < steps // 2, pl.program_id(0) >= steps // 2)):
            @pl.when(on)
            def _():
                at = 0
                for b, rows in enumerate(ms):
                    outs[2 * b + h][...] = r[at:at + rows]
                    at += rows

    w_spec = pl.BlockSpec((tile, F), lambda j: (j, 0)) if nt else pl.BlockSpec((F, tile), lambda j: (0, j))
    lo = lambda j: (0, jnp.minimum(j, steps // 2 - 1))
    hi = lambda j: (0, jnp.maximum(j - steps // 2, 0))
    blocks = [p for part in parts for p in part]
    out = pl.pallas_call(
        body, grid=(steps,),
        in_specs=[pl.BlockSpec(p.shape, lambda j: (0, 0)) for p in blocks] + [w_spec] * n + [ANY] * len(after),
        out_specs=[pl.BlockSpec((r, tile), f) for r in ms for f in (lo, hi)],
        out_shape=[jax.ShapeDtypeStruct((r, half), jnp.float32) for r in ms for _ in range(2)],
        scratch_shapes=[pltpu.VMEM((m, F), jnp.bfloat16)] * n if nb > 1 else [],
        compiler_params=_params(), cost_estimate=_cost(m, F * n, D, 4 * m * D),
        name="down",
    )(*blocks, *weights, *after)
    return [out[2 * b:2 * b + 2] for b in range(len(ms))]


def _grad(left, right, tile, after=()):
    m, N, M = sum(p.shape[0] for p in left), right[0].shape[1], left[0].shape[1]
    nl, nr = len(left), len(right)

    def body(*refs):
        ls, rs = refs[:nl], refs[nl:nl + nr]
        out, lcat, rcat = refs[-3:]
        at = 0
        for p in ls:
            lcat[at:at + p.shape[0]] = p[...]
            at += p.shape[0]
        _fill(rs, rcat)
        out[...] = _tn(lcat[...], rcat[...])

    return pl.pallas_call(
        body, grid=(M // tile,),
        in_specs=[pl.BlockSpec((p.shape[0], tile), lambda j: (0, j)) for p in left]
        + [pl.BlockSpec(p.shape, lambda j: (0, 0)) for p in right] + [ANY] * len(after),
        out_specs=pl.BlockSpec((tile, N), lambda j: (j, 0)),
        out_shape=jax.ShapeDtypeStruct((M, N), jnp.float32),
        scratch_shapes=[pltpu.VMEM((m, tile), jnp.bfloat16), pltpu.VMEM((m, N), jnp.bfloat16)],
        compiler_params=_params(), cost_estimate=_cost(M, m, N, 4 * M * N),
    )(*left, *right, *after)


def _norm(X, gamma, tile=64):
    def body(x_ref, g_ref, out):
        out[...] = (_ln(x_ref[...].astype(jnp.float32))[0] * g_ref[...]).astype(jnp.bfloat16)

    n, D = X.shape
    spec = pl.BlockSpec((tile, D), lambda j: (j, 0))
    return pl.pallas_call(
        body, grid=(n // tile,), in_specs=[spec, pl.BlockSpec((1, D), lambda j: (0, 0))], out_specs=spec,
        out_shape=jax.ShapeDtypeStruct(X.shape, X.dtype), compiler_params=_params(),
        cost_estimate=pl.CostEstimate(flops=10 * n * D, bytes_accessed=4 * n * D, transcendentals=0), name="norm",
    )(X, gamma[None])


def _finish(base, last, row, whole, n, tile=64):
    def body(*refs):
        out = refs[-1]
        half = out.shape[1] // 2
        for h in range(2):
            out[:, h * half:(h + 1) * half] = (refs[h][...] + refs[2 + h][...]).astype(out.dtype)

    rows, half = last[0].shape
    at = lambda j: (j + row // tile, 0)
    spec = pl.BlockSpec((tile, half), at)
    return pl.pallas_call(
        body, grid=(rows // tile,),
        in_specs=[spec] * 2 + [pl.BlockSpec((tile, half), lambda j: (j, 0))] * 2 + [ANY] * (whole is not None),
        out_specs=pl.BlockSpec((tile, 2 * half), at),
        out_shape=jax.ShapeDtypeStruct((n, 2 * half), jnp.bfloat16),
        input_output_aliases={4: 0} if whole is not None else {}, compiler_params=_params(),
        cost_estimate=pl.CostEstimate(flops=2 * rows * half, bytes_accessed=20 * rows * half, transcendentals=0),
        name="finish",
    )(*base, *last, *([] if whole is None else [whole]))


def _tie(vals, after):
    return lax.optimization_barrier((tuple(vals), tuple(after)))[0]


def _near(v):
    return _swap(v, XN), _swap(v, YN)


def _far(gx, gy):
    h = gx.shape[0] // 2
    sent = gy[:h], gx[h:]
    return _swap(sent[0], XN), _swap(sent[1], YN), sent


def solution(mesh):
    rows = P(("data", "tp"), None)

    def block(X, gamma, W1, W2, dY):
        n, D = X.shape
        W1p = _swap(W1, CORE)
        W2p = _swap(W2, CORE)
        x0 = _norm(X, gamma)
        xx, xy = _near(x0)
        gx, gy = _near(dY)
        Ws1, Ws2 = [W1, W1p], [W2, W2p]

        H0, s0 = _up([x0], [W1], NN)
        H0p, s0p = _up([x0], [W1p], NN, after=(H0,))
        (A0,) = _up([dY], [W2], NT, slopes=(s0,), after=(H0p,))
        (A0p,) = _up([dY], [W2p], NT, slopes=(s0p,), after=(A0,))
        xx, xy = _tie((xx, xy), (A0p,))
        xa, xb, sent = _far(xx, xy)
        Hn, sn, Hnp, snp = _up([xx, xy], Ws1, NN, after=(A0p,) + sent)
        Yx, Yy = _down([[Hn], [Hnp]], Ws2, NN, split=2)
        sa = _swap(Yx[0], XN)
        sb = _swap(Yy[1], YN)
        gx, gy = _tie((gx, gy), (Yx[0],))
        ga, gb, sent = _far(gx, gy)
        An, Anp = _up([gx, gy], Ws2, NT, slopes=(sn, snp), after=(Yx[0],) + sent)
        Zx, Zy = _down([[An], [Anp]], Ws1, NT, split=2)
        ra = _swap(Zx[0], XN)
        rb = _swap(Zy[1], YN)
        Hd, sd, Hdp, sdp = _up([xa, xb], Ws1, NN, after=(Zx[0],))
        Ad, Adp = _up([ga, gb], Ws2, NT, slopes=(sd, sdp))
        Z0, Zd = _down([[A0, Ad], [A0p, Adp]], Ws1, NT)
        fa = _swap(Zd[0], XN)
        fb = _swap(Zd[1], YN)
        Y0, Yd = _down([[H0, Hd], [H0p, Hdp]], Ws2, NN, after=(Zd[0],))
        ya = _swap(Yd[0], XN)
        yb = _swap(Yd[1], YN)
        pair = lambda own, sent: own + [_swap(v, CORE) for v in _tie(sent, (Ad,))]
        dW1 = _grad(pair([x0, xx, xy, xa, xb], [x0, xx, xy, xa, xb]),
                      pair([A0, An, Ad], [A0p, Anp, Adp]), 512, after=(Yd[0],))
        Zx1, Zy0 = _tie((Zx[1], Zy[0]), (dW1,))
        far_a, far_b = Zy0 + fa, Zx1 + fb
        za = _swap(far_a, YN)
        zb = _swap(far_b, XN)
        dW2 = _grad(pair([H0, Hn, Hd], [H0p, Hnp, Hdp]),
                      pair([dY, gx, gy, ga, gb], [dY, gx, gy, ga, gb]), 256, after=(far_a, far_b))
        Yx1, Yy0, Y00, Y01, X = _tie((Yx[1], Yy[0], Y0[0], Y0[1], X), (dW2,))
        far_a, far_b = Yy0 + ya, Yx1 + yb
        q = n - n // 4
        va = _swap(far_a[:q], YN)
        vb = _swap(far_b[:q], XN)
        x = X.astype(jnp.float32)
        base = x[:, :D // 2] + (Y00 + sa), x[:, D // 2:] + (Y01 + sb)
        xhatv, rstd = _ln(x)
        Z00, Z01 = _tie(Z0, base)
        dXn = jnp.concatenate([Z00 + ra + za, Z01 + rb + zb], axis=1)
        dg = jnp.sum(dXn * xhatv, axis=0)
        dg = dg + _swap(dg, CORE)
        dgamma = (dg + _swap(dg, XN)) + (_swap(dg, YN) + _swap(dg, DIAG))
        wa = _swap(far_a[q:], YN)
        wb = _swap(far_b[q:], XN)
        dxhat = dXn * gamma
        dx = rstd * (dxhat - jnp.mean(dxhat, axis=-1, keepdims=True) - xhatv * jnp.mean(dxhat * xhatv, axis=-1, keepdims=True))
        dX = (dY.astype(jnp.float32) + dx).astype(jnp.bfloat16)
        va, vb = _tie((va, vb), (dX,))
        Y = _finish(base, (va, vb), 0, None, n)
        Y = _finish(base, (wa, wb), q, Y, n)
        return Y, dX, dW1, dW2, dgamma

    return jax.shard_map(block, mesh=mesh,
                         in_specs=(rows, P(None), P(None, "tp"), P("tp", None), rows),
                         out_specs=(rows, rows, P("data", "tp"), rows, P("data")),
                         check_vma=False)
```

```python
import jax
import jax.numpy as jnp
from jax import lax
from jax.experimental import pallas as pl
from jax.experimental.pallas import tpu as pltpu
from jax.sharding import PartitionSpec as P


EPS = 1e-6


CORE, XN, YN, DIAG = 1, 2, 4, 6
NN = (((1,), (0,)), ((), ()))
NT = (((1,), (1,)), ((), ()))
ANY = pl.BlockSpec(memory_space=pl.ANY)


C1, C2 = 0.7978845608028654, 0.7978845608028654 * 0.044715


def _gelu(a):
    s = a * a
    q = 0.5 + 0.5 * jnp.tanh(a * (C1 + C2 * s))
    h = a * q
    return h, q + (h - h * q) * (2 * C1 + (6 * C2) * s)


def _ln(x):
    mu = jnp.mean(x, axis=-1, keepdims=True)
    xc = x - mu
    var = jnp.mean(xc * xc, axis=-1, keepdims=True)
    rstd = lax.rsqrt(var + EPS)
    return xc * rstd, rstd


def _tn(a, b):
    return lax.dot_general(a, b, (((0,), (0,)), ((), ())), preferred_element_type=jnp.float32)


def _dot(a, b, dims):
    return lax.dot_general(a, b, dims, preferred_element_type=jnp.float32)


def _swap(v, k):
    return lax.ppermute(v, "tp", [(i, i ^ k) for i in range(8)])


def _cost(m, k, n, extra=0):
    return pl.CostEstimate(flops=2 * m * k * n, bytes_accessed=2 * k * n + 2 * m * k + extra, transcendentals=0)


def _params():
    return pltpu.CompilerParams(dimension_semantics=("arbitrary",), vmem_limit_bytes=60 << 20)


def _fill(pieces, cat):
    if cat is None:
        return pieces[0][...]

    @pl.when(pl.program_id(0) == 0)
    def _():
        at = 0
        for p in pieces:
            cat[at:at + p.shape[0]] = p[...]
            at += p.shape[0]

    return cat[...]


def _norm(pieces, gamma, out, chunk=32):
    at = 0
    for p in pieces:
        def rows(i, _, p=p, at=at):
            r = pl.multiple_of(i * chunk, chunk)
            xhatv, _ = _ln(p[pl.ds(r, chunk)].astype(jnp.float32))
            out[pl.ds(at + r, chunk)] = (xhatv * gamma[...]).astype(out.dtype)
            return 0

        lax.fori_loop(0, p.shape[0] // chunk, rows, 0)
        at += p.shape[0]


def _up(pieces, weights, dims, slopes=None, gamma=None, after=(), tile=256):
    m, D = sum(p.shape[0] for p in pieces), pieces[0].shape[1]
    nt = dims == NT
    F = weights[0].shape[0 if nt else 1]
    nw, npc, ns, nx = len(weights), len(pieces), len(slopes or ()), int(gamma is not None)

    def body(*refs):
        ps, ws, ss = refs[:npc], refs[npc:npc + nw], refs[npc + nw:npc + nw + ns]
        outs = refs[npc + nw + ns + nx + len(after):]
        if nx:
            @pl.when(pl.program_id(0) == 0)
            def _():
                _norm(ps, refs[npc + nw + ns], outs[-1])

            a = outs[-1][...]
        else:
            a = _fill(ps, refs[-1] if npc > 1 else None)
        for i in range(nw):
            r = _dot(a, ws[i][...], dims)
            if slopes:
                outs[i][...] = (ss[i][...] * r).astype(jnp.bfloat16)
            else:
                h, slope = _gelu(r)
                outs[2 * i][...] = h.astype(jnp.bfloat16)
                outs[2 * i + 1][...] = slope

    w_spec = pl.BlockSpec((tile, D), lambda j: (j, 0)) if nt else pl.BlockSpec((D, tile), lambda j: (0, j))
    o_spec = pl.BlockSpec((m, tile), lambda j: (0, j))
    types = [jnp.bfloat16] * nw if slopes else [jnp.bfloat16, jnp.float32] * nw
    return pl.pallas_call(
        body, grid=(F // tile,),
        in_specs=[pl.BlockSpec(p.shape, lambda j: (0, 0)) for p in pieces] + [w_spec] * nw
        + [o_spec] * ns + [pl.BlockSpec((1, D), lambda j: (0, 0))] * nx + [ANY] * len(after),
        out_specs=[o_spec] * len(types) + [pl.BlockSpec((m, D), lambda j: (0, 0))] * nx,
        out_shape=[jax.ShapeDtypeStruct((m, F), t) for t in types] + [jax.ShapeDtypeStruct((m, D), jnp.bfloat16)] * nx,
        scratch_shapes=[pltpu.VMEM((m, D), jnp.bfloat16)] if npc > 1 and not nx else [],
        compiler_params=_params(), cost_estimate=_cost(m, D, F * nw),
        name="up_dA" if slopes else "up_A",
    )(*pieces, *weights, *(slopes or ()), *([gamma[None]] if nx else []), *after)


def _down(parts, weights, dims, split=1, after=(), tile=512):
    F = parts[0][0].shape[1]
    m, nb = sum(p.shape[0] for p in parts[0]), len(parts[0])
    ms = [p.shape[0] // split for p in parts[0] for _ in range(split)]
    nt = dims == NT
    D = weights[0].shape[0 if nt else 1]
    n = len(parts)
    half, steps = D // 2, D // tile
    nin = n * nb

    def body(*refs):
        ws, outs = refs[nin:nin + n], refs[nin + n + len(after):]
        cats = outs[2 * len(ms):] or [None] * n
        r = None
        for i in range(n):
            d = _dot(_fill(refs[i * nb:(i + 1) * nb], cats[i]), ws[i][...], dims)
            r = d if r is None else r + d

        for h, on in enumerate((pl.program_id(0) < steps // 2, pl.program_id(0) >= steps // 2)):
            @pl.when(on)
            def _():
                at = 0
                for b, rows in enumerate(ms):
                    outs[2 * b + h][...] = r[at:at + rows]
                    at += rows

    w_spec = pl.BlockSpec((tile, F), lambda j: (j, 0)) if nt else pl.BlockSpec((F, tile), lambda j: (0, j))
    lo = lambda j: (0, jnp.minimum(j, steps // 2 - 1))
    hi = lambda j: (0, jnp.maximum(j - steps // 2, 0))
    blocks = [p for part in parts for p in part]
    out = pl.pallas_call(
        body, grid=(steps,),
        in_specs=[pl.BlockSpec(p.shape, lambda j: (0, 0)) for p in blocks] + [w_spec] * n + [ANY] * len(after),
        out_specs=[pl.BlockSpec((r, tile), f) for r in ms for f in (lo, hi)],
        out_shape=[jax.ShapeDtypeStruct((r, half), jnp.float32) for r in ms for _ in range(2)],
        scratch_shapes=[pltpu.VMEM((m, F), jnp.bfloat16)] * n if nb > 1 else [],
        compiler_params=_params(), cost_estimate=_cost(m, F * n, D, 4 * m * D),
        name="down",
    )(*blocks, *weights, *after)
    return [out[2 * b:2 * b + 2] for b in range(len(ms))]


def _grad(left, right, tile, after=()):
    m, N, M = sum(p.shape[0] for p in left), right[0].shape[1], left[0].shape[1]
    nl, nr = len(left), len(right)

    def body(*refs):
        ls, rs = refs[:nl], refs[nl:nl + nr]
        out, lcat, rcat = refs[-3:]
        at = 0
        for p in ls:
            lcat[at:at + p.shape[0]] = p[...]
            at += p.shape[0]
        _fill(rs, rcat)
        out[...] = _tn(lcat[...], rcat[...])

    return pl.pallas_call(
        body, grid=(M // tile,),
        in_specs=[pl.BlockSpec((p.shape[0], tile), lambda j: (0, j)) for p in left]
        + [pl.BlockSpec(p.shape, lambda j: (0, 0)) for p in right] + [ANY] * len(after),
        out_specs=pl.BlockSpec((tile, N), lambda j: (j, 0)),
        out_shape=jax.ShapeDtypeStruct((M, N), jnp.float32),
        scratch_shapes=[pltpu.VMEM((m, tile), jnp.bfloat16), pltpu.VMEM((m, N), jnp.bfloat16)],
        compiler_params=_params(), cost_estimate=_cost(M, m, N, 4 * M * N),
    )(*left, *right, *after)


def _finish(base, last, row, whole, n, tile):
    def body(*refs):
        out = refs[-1]
        half = out.shape[1] // 2
        for h in range(2):
            out[:, h * half:(h + 1) * half] = (refs[h][...] + refs[2 + h][...]).astype(out.dtype)

    rows, half = last[0].shape
    at = lambda j: (j + row // tile, 0)
    spec = pl.BlockSpec((tile, half), at)
    return pl.pallas_call(
        body, grid=(rows // tile,),
        in_specs=[spec] * 2 + [pl.BlockSpec((tile, half), lambda j: (j, 0))] * 2 + [ANY] * (whole is not None),
        out_specs=pl.BlockSpec((tile, 2 * half), at),
        out_shape=jax.ShapeDtypeStruct((n, 2 * half), jnp.bfloat16),
        input_output_aliases={4: 0} if whole is not None else {}, compiler_params=_params(),
        cost_estimate=pl.CostEstimate(flops=2 * rows * half, bytes_accessed=20 * rows * half, transcendentals=0),
        name="finish",
    )(*base, *last, *([] if whole is None else [whole]))


def _tie(vals, after):
    return lax.optimization_barrier((tuple(vals), tuple(after)))[0]


def _near(v):
    return _swap(v, XN), _swap(v, YN)


def solution(mesh):
    rows = P(("data", "tp"), None)

    def block(X, gamma, W1, W2, dY):
        n, D = X.shape
        xx, xy = _near(X)
        gx, gy = _near(dY)
        W1p = _swap(W1, CORE)
        W2p = _swap(W2, CORE)
        Ws1, Ws2 = [W1, W1p], [W2, W2p]

        H0, s0, X0 = _up([X], [W1], NN, gamma=gamma)
        (A0,) = _up([dY], [W2], NT, slopes=(s0,))
        H0p, s0p, _ = _up([X], [W1p], NN, gamma=gamma, after=(A0,))
        xx, xy = _tie((xx, xy), (H0p,))
        xd = _swap(xy, XN)
        Hn, sn, Hnp, snp, Xn = _up([xx, xy], Ws1, NN, gamma=gamma, after=(H0p,))
        (A0p,) = _up([dY], [W2p], NT, slopes=(s0p,), after=(Hn,))
        gx, gy = _tie((gx, gy), (A0p,))
        gd = _swap(gx, YN)
        Yx, Yy = _down([[Hn], [Hnp]], Ws2, NN, split=2, after=(A0p,))
        sa = _swap(Yx[0], XN)
        sb = _swap(Yy[1], YN)
        An, Anp = _up([gx, gy], Ws2, NT, slopes=(sn, snp), after=(Yx[0],))
        Zx, Zy = _down([[An], [Anp]], Ws1, NT, split=2)
        ra = _swap(Zx[0], XN)
        rb = _swap(Zy[1], YN)
        Hd, sd, Hdp, sdp, Xd = _up([xd], Ws1, NN, gamma=gamma, after=(Zx[0],))
        Ad, Adp = _up([gd], Ws2, NT, slopes=(sd, sdp))
        (Zd,) = _down([[Ad], [Adp]], Ws1, NT)
        fa = _swap(Zd[0], XN)
        fb = _swap(Zd[1], YN)
        Y0, Yd = _down([[H0, Hd], [H0p, Hdp]], Ws2, NN, after=(Zd[0],))
        ya = _swap(Yd[0], XN)
        yb = _swap(Yd[1], YN)
        pair = lambda own, sent: own + [_swap(v, CORE) for v in _tie(sent, (Ad,))]
        dW1 = _grad(pair([X0, Xn, Xd], [X0, Xn, Xd]),
                      pair([A0, An, Ad], [A0p, Anp, Adp]), 512, after=(Yd[0],))
        Zx1, Zy0 = _tie((Zx[1], Zy[0]), (dW1,))
        far_a, far_b = Zy0 + fa, Zx1 + fb
        za = _swap(far_a, YN)
        zb = _swap(far_b, XN)
        dW2 = _grad(pair([H0, Hn, Hd], [H0p, Hnp, Hdp]),
                      pair([dY, gx, gy, gd], [dY, gx, gy, gd]), 256, after=(far_a, far_b))
        Yx1, Yy0, Y00, Y01, X = _tie((Yx[1], Yy[0], Y0[0], Y0[1], X), (dW2,))
        far_a, far_b = Yy0 + ya, Yx1 + yb
        q = n - n // 8
        va = _swap(far_a[:q], YN)
        vb = _swap(far_b[:q], XN)
        x = X.astype(jnp.float32)
        base = x[:, :D // 2] + (Y00 + sa), x[:, D // 2:] + (Y01 + sb)
        xhatv, rstd = _ln(x)
        (Z0,) = _down([[A0], [A0p]], Ws1, NT, after=base)
        dXn = jnp.concatenate([Z0[0] + ra + za, Z0[1] + rb + zb], axis=1)
        dg = jnp.sum(dXn * xhatv, axis=0)
        dg = dg + _swap(dg, CORE)
        dgamma = (dg + _swap(dg, XN)) + (_swap(dg, YN) + _swap(dg, DIAG))
        wa = _swap(far_a[q:], YN)
        wb = _swap(far_b[q:], XN)
        dxhat = dXn * gamma
        dx = rstd * (dxhat - jnp.mean(dxhat, axis=-1, keepdims=True) - xhatv * jnp.mean(dxhat * xhatv, axis=-1, keepdims=True))
        dX = (dY.astype(jnp.float32) + dx).astype(jnp.bfloat16)
        va, vb = _tie((va, vb), (dX,))
        Y = _finish(base, (va, vb), 0, None, n, q // 2)
        Y = _finish(base, (wa, wb), q, Y, n, n - q)
        return Y, dX, dW1, dW2, dgamma

    return jax.shard_map(block, mesh=mesh,
                         in_specs=(rows, P(None), P(None, "tp"), P("tp", None), rows),
                         out_specs=(rows, rows, P("data", "tp"), rows, P("data")),
                         check_vma=False)
```

```python
import jax
import jax.numpy as jnp
from jax import lax
from jax.experimental import pallas as pl
from jax.experimental.pallas import tpu as pltpu
from jax.sharding import PartitionSpec as P


EPS = 1e-6


CORE, XN, YN, DIAG = 1, 2, 4, 6
NN = (((1,), (0,)), ((), ()))
NT = (((1,), (1,)), ((), ()))
ANY = pl.BlockSpec(memory_space=pl.ANY)


C1, C2 = 0.7978845608028654, 0.7978845608028654 * 0.044715


def _gelu(a):
    s = a * a
    q = 0.5 + 0.5 * jnp.tanh(a * (C1 + C2 * s))
    h = a * q
    return h, q + (h - h * q) * (2 * C1 + (6 * C2) * s)


def _ln(x):
    mu = jnp.mean(x, axis=-1, keepdims=True)
    xc = x - mu
    var = jnp.mean(xc * xc, axis=-1, keepdims=True)
    rstd = lax.rsqrt(var + EPS)
    return xc * rstd, rstd


def _tn(a, b):
    return lax.dot_general(a, b, (((0,), (0,)), ((), ())), preferred_element_type=jnp.float32)


def _dot(a, b, dims):
    return lax.dot_general(a, b, dims, preferred_element_type=jnp.float32)


def _swap(v, k):
    return lax.ppermute(v, "tp", [(i, i ^ k) for i in range(8)])


def _cost(m, k, n, extra=0):
    return pl.CostEstimate(flops=2 * m * k * n, bytes_accessed=2 * k * n + 2 * m * k + extra, transcendentals=0)


def _params():
    return pltpu.CompilerParams(dimension_semantics=("arbitrary",), vmem_limit_bytes=67_000_000)


def _fill(pieces, cat):
    if cat is None:
        return pieces[0][...]

    @pl.when(pl.program_id(0) == 0)
    def _():
        at = 0
        for p in pieces:
            cat[at:at + p.shape[0]] = p[...]
            at += p.shape[0]

    return cat[...]


def _norm(pieces, gamma, out, chunk=16):
    at = 0
    for p in pieces:
        def rows(i, _, p=p, at=at):
            r = pl.multiple_of(i * chunk, chunk)
            xhatv, _ = _ln(p[pl.ds(r, chunk)].astype(jnp.float32))
            out[pl.ds(at + r, chunk)] = (xhatv * gamma[...]).astype(out.dtype)
            return 0

        lax.fori_loop(0, p.shape[0] // chunk, rows, 0, unroll=4)
        at += p.shape[0]


def _up(pieces, weights, dims, slopes=None, gamma=None, after=(), tile=256):
    m, D = sum(p.shape[0] for p in pieces), pieces[0].shape[1]
    nt = dims == NT
    F = weights[0].shape[0 if nt else 1]
    nw, npc, ns, nx = len(weights), len(pieces), len(slopes or ()), int(gamma is not None)

    def body(*refs):
        ps, ws, ss = refs[:npc], refs[npc:npc + nw], refs[npc + nw:npc + nw + ns]
        outs = refs[npc + nw + ns + nx + len(after):]
        if nx:
            @pl.when(pl.program_id(0) == 0)
            def _():
                _norm(ps, refs[npc + nw + ns], outs[-1])

            a = outs[-1][...]
        else:
            a = _fill(ps, refs[-1] if npc > 1 else None)
        for i in range(nw):
            r = _dot(a, ws[i][...], dims)
            if slopes:
                outs[i][...] = (ss[i][...] * r).astype(jnp.bfloat16)
            else:
                h, slope = _gelu(r)
                outs[2 * i][...] = h.astype(jnp.bfloat16)
                outs[2 * i + 1][...] = slope

    w_spec = pl.BlockSpec((tile, D), lambda j: (j, 0)) if nt else pl.BlockSpec((D, tile), lambda j: (0, j))
    o_spec = pl.BlockSpec((m, tile), lambda j: (0, j))
    types = [jnp.bfloat16] * nw if slopes else [jnp.bfloat16, jnp.float32] * nw
    return pl.pallas_call(
        body, grid=(F // tile,),
        in_specs=[pl.BlockSpec(p.shape, lambda j: (0, 0)) for p in pieces] + [w_spec] * nw
        + [o_spec] * ns + [pl.BlockSpec((1, D), lambda j: (0, 0))] * nx + [ANY] * len(after),
        out_specs=[o_spec] * len(types) + [pl.BlockSpec((m, D), lambda j: (0, 0))] * nx,
        out_shape=[jax.ShapeDtypeStruct((m, F), t) for t in types] + [jax.ShapeDtypeStruct((m, D), jnp.bfloat16)] * nx,
        scratch_shapes=[pltpu.VMEM((m, D), jnp.bfloat16)] if npc > 1 and not nx else [],
        compiler_params=_params(), cost_estimate=_cost(m, D, F * nw),
        name="up_dA" if slopes else "up_A",
    )(*pieces, *weights, *(slopes or ()), *([gamma[None]] if nx else []), *after)


def _down(parts, weights, dims, split=1, halves=(0, 1), after=(), tile=512):
    F = parts[0][0].shape[1]
    m, nb = sum(p.shape[0] for p in parts[0]), len(parts[0])
    ms = [p.shape[0] // split for p in parts[0] for _ in range(split)]
    nt = dims == NT
    D = weights[0].shape[0 if nt else 1]
    n = len(parts)
    half, nh = D // 2, len(halves)
    per = half // tile
    steps, off = nh * per, halves[0] * per
    nin = n * nb

    def body(*refs):
        ws, outs = refs[nin:nin + n], refs[nin + n + len(after):]
        cats = outs[nh * len(ms):] or [None] * n
        r = None
        for i in range(n):
            d = _dot(_fill(refs[i * nb:(i + 1) * nb], cats[i]), ws[i][...], dims)
            r = d if r is None else r + d

        for h in range(nh):
            @pl.when(pl.program_id(0) // per == h)
            def _():
                at = 0
                for b, rows in enumerate(ms):
                    outs[nh * b + h][...] = r[at:at + rows]
                    at += rows

    w_spec = pl.BlockSpec((tile, F), lambda j: (j + off, 0)) if nt else pl.BlockSpec((F, tile), lambda j: (0, j + off))
    places = [lambda j, h=h: (0, jnp.clip(j - h * per, 0, per - 1)) for h in range(nh)]
    blocks = [p for part in parts for p in part]
    out = pl.pallas_call(
        body, grid=(steps,),
        in_specs=[pl.BlockSpec(p.shape, lambda j: (0, 0)) for p in blocks] + [w_spec] * n + [ANY] * len(after),
        out_specs=[pl.BlockSpec((r, tile), f) for r in ms for f in places],
        out_shape=[jax.ShapeDtypeStruct((r, half), jnp.float32) for r in ms for _ in halves],
        scratch_shapes=[pltpu.VMEM((m, F), jnp.bfloat16)] * n if nb > 1 else [],
        compiler_params=_params(), cost_estimate=_cost(m, F * n, nh * half, 4 * m * nh * half),
        name="down",
    )(*blocks, *weights, *after)
    return [out[nh * b:nh * (b + 1)] for b in range(len(ms))]


def _grad(left, right, tile, after=()):
    m, N, M = sum(p.shape[0] for p in left), right[0].shape[1], left[0].shape[1]
    nl, nr = len(left), len(right)

    def body(*refs):
        ls, rs = refs[:nl], refs[nl:nl + nr]
        out, lcat, rcat = refs[-3:]
        at = 0
        for p in ls:
            lcat[at:at + p.shape[0]] = p[...]
            at += p.shape[0]
        _fill(rs, rcat)
        out[...] = _tn(lcat[...], rcat[...])

    return pl.pallas_call(
        body, grid=(M // tile,),
        in_specs=[pl.BlockSpec((p.shape[0], tile), lambda j: (0, j)) for p in left]
        + [pl.BlockSpec(p.shape, lambda j: (0, 0)) for p in right] + [ANY] * len(after),
        out_specs=pl.BlockSpec((tile, N), lambda j: (j, 0)),
        out_shape=jax.ShapeDtypeStruct((M, N), jnp.float32),
        scratch_shapes=[pltpu.VMEM((m, tile), jnp.bfloat16), pltpu.VMEM((m, N), jnp.bfloat16)],
        compiler_params=_params(), cost_estimate=_cost(M, m, N, 4 * M * N),
    )(*left, *right, *after)


def _finish(base, last, row, whole, n, tile, dgs=()):
    nw, ng = int(whole is not None), len(dgs)

    def body(*refs):
        gs, outs = refs[4:4 + ng], refs[4 + ng + nw:]
        half = outs[0].shape[1] // 2
        for h in range(2):
            outs[0][:, h * half:(h + 1) * half] = (refs[h][...] + refs[2 + h][...]).astype(outs[0].dtype)
        if ng:
            outs[1][...] = (gs[0][...] + gs[1][...]) + (gs[2][...] + gs[3][...])

    rows, half = last[0].shape
    at = lambda j: (j + row // tile, 0)
    spec = pl.BlockSpec((tile, half), at)
    one = pl.BlockSpec((1, 2 * half), lambda j: (0, 0))
    out = pl.pallas_call(
        body, grid=(rows // tile,),
        in_specs=[spec] * 2 + [pl.BlockSpec((tile, half), lambda j: (j, 0))] * 2 + [one] * ng + [ANY] * nw,
        out_specs=[pl.BlockSpec((tile, 2 * half), at)] + [one] * bool(ng),
        out_shape=[jax.ShapeDtypeStruct((n, 2 * half), jnp.bfloat16)] + [jax.ShapeDtypeStruct((1, 2 * half), jnp.float32)] * bool(ng),
        input_output_aliases={4 + ng: 0} if nw else {}, compiler_params=_params(),
        cost_estimate=pl.CostEstimate(flops=2 * rows * half, bytes_accessed=20 * rows * half, transcendentals=0),
        name="finish",
    )(*base, *last, *dgs, *([whole] if nw else []))
    return out if ng else out[0]


def _sums(pairs, pieces, tile):
    n, D = pairs[0][0].shape
    starts = [sum(pieces[:i]) // tile for i in range(len(pieces) + 1)]

    def body(*refs):
        ins, outs = refs[:2 * len(pairs)], refs[2 * len(pairs):]
        j = pl.program_id(0)
        for i in range(len(pairs)):
            r = ins[2 * i][...] + ins[2 * i + 1][...]
            for h in range(len(pieces)):
                @pl.when((j >= starts[h]) & (j < starts[h + 1]))
                def _():
                    outs[len(pieces) * i + h][...] = r

    spec = pl.BlockSpec((tile, D), lambda j: (j, 0))
    outs = [pl.BlockSpec((tile, D), lambda j, lo=lo, hi=hi: (jnp.clip(j - lo, 0, hi - lo - 1), 0))
            for lo, hi in zip(starts, starts[1:])]
    return pl.pallas_call(
        body, grid=(n // tile,), in_specs=[spec] * (2 * len(pairs)), out_specs=outs * len(pairs),
        out_shape=[jax.ShapeDtypeStruct((r, D), jnp.float32) for r in pieces] * len(pairs), compiler_params=_params(),
        cost_estimate=pl.CostEstimate(flops=2 * n * D, bytes_accessed=24 * n * D, transcendentals=0),
    )(*[v for p in pairs for v in p])


def _base(X, terms, tile=64):
    n, D = X.shape
    half = D // 2

    def body(x_ref, *refs):
        for h in range(2):
            x = x_ref[:, h * half:(h + 1) * half].astype(jnp.float32)
            refs[4 + h][...] = x + (refs[2 * h][...] + refs[2 * h + 1][...])

    spec = pl.BlockSpec((tile, half), lambda j: (j, 0))
    return pl.pallas_call(
        body, grid=(n // tile,), in_specs=[pl.BlockSpec((tile, D), lambda j: (j, 0))] + [spec] * 4, out_specs=[spec] * 2,
        out_shape=[jax.ShapeDtypeStruct((n, half), jnp.float32)] * 2, compiler_params=_params(),
        cost_estimate=pl.CostEstimate(flops=2 * n * D, bytes_accessed=14 * n * D, transcendentals=0), name="base",
    )(X, *[v for t in terms for v in t])


def _dx(terms, X, dY, gamma, tile=64):
    n, D = X.shape
    nt = len(terms[0])

    def body(x_ref, dy_ref, g_ref, *refs):
        ts, (out, dg) = refs[:2 * nt], refs[2 * nt:]
        halves = []
        for h in range(2):
            v = ts[h * nt][...]
            for t in ts[h * nt + 1:(h + 1) * nt]:
                v = v + t[...]
            halves.append(v)
        dXn = jnp.concatenate(halves, axis=1)
        xhatv, rstd = _ln(x_ref[...].astype(jnp.float32))
        part = jnp.sum(dXn * xhatv, axis=0, keepdims=True)

        @pl.when(pl.program_id(0) == 0)
        def _():
            dg[...] = part

        @pl.when(pl.program_id(0) > 0)
        def _():
            dg[...] += part

        dxhat = dXn * g_ref[...]
        dx = rstd * (dxhat - jnp.mean(dxhat, axis=-1, keepdims=True) - xhatv * jnp.mean(dxhat * xhatv, axis=-1, keepdims=True))
        out[...] = (dy_ref[...].astype(jnp.float32) + dx).astype(out.dtype)

    row = pl.BlockSpec((tile, D), lambda j: (j, 0))
    one = pl.BlockSpec((1, D), lambda j: (0, 0))
    return pl.pallas_call(
        body, grid=(n // tile,),
        in_specs=[row, row, one] + [pl.BlockSpec((tile, D // 2), lambda j: (j, 0))] * (2 * nt),
        out_specs=[row, one],
        out_shape=[jax.ShapeDtypeStruct((n, D), jnp.bfloat16), jax.ShapeDtypeStruct((1, D), jnp.float32)],
        compiler_params=_params(),
        cost_estimate=pl.CostEstimate(flops=20 * n * D, bytes_accessed=(6 + 4 * nt) * n * D, transcendentals=0),
        name="dx",
    )(X, dY, gamma[None], *terms[0], *terms[1])


def _halves(v):
    n, D = v.shape

    def body(ref, lo, hi):
        for h, out in enumerate((lo, hi)):
            @pl.when(pl.program_id(0) == h)
            def _():
                out[...] = ref[...]

    return pl.pallas_call(
        body, grid=(2,), in_specs=[pl.BlockSpec((n // 2, D), lambda j: (j, 0))],
        out_specs=[pl.BlockSpec((n // 2, D), lambda j: (0, 0))] * 2,
        out_shape=[jax.ShapeDtypeStruct((n // 2, D), v.dtype)] * 2, compiler_params=_params(),
        cost_estimate=pl.CostEstimate(flops=n * D, bytes_accessed=4 * n * D, transcendentals=0), name="halves",
    )(v)


def _tie(vals, after):
    return lax.optimization_barrier((tuple(vals), tuple(after)))[0]


def _near(v):
    return _swap(v, XN), _swap(v, YN)


def solution(mesh):
    rows = P(("data", "tp"), None)

    def block(X, gamma, W1, W2, dY):
        n, D = X.shape
        xx, xy = _near(X)
        W1p = _swap(W1, CORE)
        halves = _halves(dY)
        gx1, gy1 = _near(halves[0])
        gx2, gy2 = _near(halves[1])
        W2p = _swap(W2, CORE)
        Ws1, Ws2 = [W1, W1p], [W2, W2p]

        H0, s0, X0 = _up([X], [W1], NN, gamma=gamma)
        (A0,) = _up([dY], [W2], NT, slopes=(s0,))
        H0p, s0p, _ = _up([X], [W1p], NN, gamma=gamma, after=(A0,))
        xx, xy = _tie((xx, xy), (H0p,))
        xd = _swap(xx, YN)
        Hn, sn, Hnp, snp, Xn = _up([xx, xy], Ws1, NN, gamma=gamma, after=(H0p,))
        gx1, gy1 = _tie((gx1, gy1), (Hn,))
        gd1 = _swap(gy1, XN)
        (Yxa,), (Yya,) = _down([[Hn], [Hnp]], Ws2, NN, split=2, halves=(0,))
        gx2, gy2 = _tie((gx2, gy2), (Yxa,))
        gd2 = _swap(gy2, XN)
        (Yxb,), (Yyb,) = _down([[Hn], [Hnp]], Ws2, NN, split=2, halves=(1,), after=(Yxa,))
        Yx, Yy = (Yxa, Yxb), (Yya, Yyb)
        sa = _swap(Yx[0], XN)
        sb = _swap(Yy[1], YN)
        An, Anp = _up([gx1, gx2, gy1, gy2], Ws2, NT, slopes=(sn, snp), after=(Yxb,))
        Zx, Zy = _down([[An], [Anp]], Ws1, NT, split=2)
        ra = _swap(Zx[0], XN)
        rb = _swap(Zy[1], YN)
        Hd, sd, Hdp, sdp, Xd = _up([xd], Ws1, NN, gamma=gamma, after=(Zx[0],))
        Ad, Adp = _up([gd1, gd2], Ws2, NT, slopes=(sd, sdp))
        (Zd,) = _down([[Ad], [Adp]], Ws1, NT)
        fa = _swap(Zd[0], XN)
        fb = _swap(Zd[1], YN)
        (A0p,) = _up([dY], [W2p], NT, slopes=(s0p,), after=(Zd[0],))
        Y0, Yd = _down([[H0, Hd], [H0p, Hdp]], Ws2, NN, after=(A0p,))
        ya = _swap(Yd[0], XN)
        yb = _swap(Yd[1], YN)
        pair = lambda own, sent: own + [_swap(v, CORE) for v in _tie(sent, (Ad,))]
        dW1 = _grad(pair([X0, Xn, Xd], [X0, Xn, Xd]),
                      pair([A0, An, Ad], [A0p, Anp, Adp]), 512, after=(Yd[0],))
        Zx1, Zy0 = _tie((Zx[1], Zy[0]), (dW1,))
        far_a, far_b = _sums(((Zy0, fa), (Zx1, fb)), (n,), 64)
        za = _swap(far_a, YN)
        zb = _swap(far_b, XN)
        Gs = [dY, gx1, gx2, gy1, gy2, gd1, gd2]
        dW2 = _grad(pair([H0, Hn, Hd], [H0p, Hnp, Hdp]),
                      pair(Gs, Gs), 256, after=(far_a, far_b))
        Yx1, Yy0, Y00, Y01, X = _tie((Yx[1], Yy[0], Y0[0], Y0[1], X), (dW2,))
        cuts = n * 5 // 8, n // 4, n // 8
        sums = _sums(((Yy0, ya), (Yx1, yb)), cuts, n // 8)
        va, vb = _swap(sums[0], YN), _swap(sums[3], XN)
        ua, ub = _swap(sums[1], YN), _swap(sums[4], XN)
        base = _base(X, ((Y00, sa), (Y01, sb)))
        (Z0,) = _down([[A0], [A0p]], Ws1, NT, after=base)
        dX, dg = _dx(((Z0[0], ra, za), (Z0[1], rb, zb)), X, dY, gamma)
        dg = dg + _swap(dg, CORE)
        dgs = dg, _swap(dg, XN), _swap(dg, YN), _swap(dg, DIAG)
        last_a, last_b = _tie((sums[2], sums[5]), (dX,))
        wa = _swap(last_a, YN)
        wb = _swap(last_b, XN)
        Y = _finish(base, (va, vb), 0, None, n, cuts[0] // 2)
        Y = _finish(base, (ua, ub), cuts[0], Y, n, cuts[2])
        Y, dgamma = _finish(base, (wa, wb), cuts[0] + cuts[1], Y, n, cuts[2], dgs)
        return Y, dX, dW1, dW2, dgamma.reshape(D)

    return jax.shard_map(block, mesh=mesh,
                         in_specs=(rows, P(None), P(None, "tp"), P("tp", None), rows),
                         out_specs=(rows, rows, P("data", "tp"), rows, P("data")),
                         check_vma=False)
```

```python
import jax
import jax.numpy as jnp
from jax import lax
from jax.experimental import pallas as pl
from jax.experimental.pallas import tpu as pltpu
from jax.sharding import PartitionSpec as P


EPS = 1e-6


CORE, XN, YN, DIAG = 1, 2, 4, 6
NN = (((1,), (0,)), ((), ()))
NT = (((1,), (1,)), ((), ()))
ANY = pl.BlockSpec(memory_space=pl.ANY)


C1, C2 = 0.7978845608028654, 0.7978845608028654 * 0.044715


def _gelu(a):
    s = a * a
    q = 0.5 + 0.5 * jnp.tanh(a * (C1 + C2 * s))
    h = a * q
    return h, q + (h - h * q) * (2 * C1 + (6 * C2) * s)


def _ln(x):
    mu = jnp.mean(x, axis=-1, keepdims=True)
    xc = x - mu
    var = jnp.mean(xc * xc, axis=-1, keepdims=True)
    rstd = lax.rsqrt(var + EPS)
    return xc * rstd, rstd


def _tn(a, b):
    return lax.dot_general(a, b, (((0,), (0,)), ((), ())), preferred_element_type=jnp.float32)


def _dot(a, b, dims):
    return lax.dot_general(a, b, dims, preferred_element_type=jnp.float32)


def _swap(v, k):
    return lax.ppermute(v, "tp", [(i, i ^ k) for i in range(8)])


def _cross(v, k):
    return lax.ppermute(v, "tp", [(i, i ^ (k if i % 2 else k ^ DIAG)) for i in range(8)])


def _cost(m, k, n, extra=0):
    return pl.CostEstimate(flops=2 * m * k * n, bytes_accessed=2 * k * n + 2 * m * k + extra, transcendentals=0)


def _params():
    return pltpu.CompilerParams(dimension_semantics=("arbitrary",), vmem_limit_bytes=67_000_000)


def _fill(pieces, cat):
    if cat is None:
        return pieces[0][...]

    @pl.when(pl.program_id(0) == 0)
    def _():
        at = 0
        for p in pieces:
            cat[at:at + p.shape[0]] = p[...]
            at += p.shape[0]

    return cat[...]


def _norm(pieces, gamma, out, chunk=16):
    at = 0
    for p in pieces:
        def rows(i, _, p=p, at=at):
            r = pl.multiple_of(i * chunk, chunk)
            xhatv, _ = _ln(p[pl.ds(r, chunk)].astype(jnp.float32))
            out[pl.ds(at + r, chunk)] = (xhatv * gamma[...]).astype(out.dtype)
            return 0

        lax.fori_loop(0, p.shape[0] // chunk, rows, 0, unroll=4)
        at += p.shape[0]


def _up(pieces, weights, dims, slopes=None, gamma=None, after=(), tile=256):
    m, D = sum(p.shape[0] for p in pieces), pieces[0].shape[1]
    nt = dims == NT
    F = weights[0].shape[0 if nt else 1]
    nw, npc, ns, nx = len(weights), len(pieces), len(slopes or ()), int(gamma is not None)

    def body(*refs):
        ps, ws, ss = refs[:npc], refs[npc:npc + nw], refs[npc + nw:npc + nw + ns]
        outs = refs[npc + nw + ns + nx + len(after):]
        if nx:
            @pl.when(pl.program_id(0) == 0)
            def _():
                _norm(ps, refs[npc + nw + ns], outs[-1])

            a = outs[-1][...]
        else:
            a = _fill(ps, refs[-1] if npc > 1 else None)
        for i in range(nw):
            r = _dot(a, ws[i][...], dims)
            if slopes:
                outs[i][...] = (ss[i][...] * r).astype(jnp.bfloat16)
            else:
                h, slope = _gelu(r)
                outs[2 * i][...] = h.astype(jnp.bfloat16)
                outs[2 * i + 1][...] = slope

    w_spec = pl.BlockSpec((tile, D), lambda j: (j, 0)) if nt else pl.BlockSpec((D, tile), lambda j: (0, j))
    o_spec = pl.BlockSpec((m, tile), lambda j: (0, j))
    types = [jnp.bfloat16] * nw if slopes else [jnp.bfloat16, jnp.float32] * nw
    return pl.pallas_call(
        body, grid=(F // tile,),
        in_specs=[pl.BlockSpec(p.shape, lambda j: (0, 0)) for p in pieces] + [w_spec] * nw
        + [o_spec] * ns + [pl.BlockSpec((1, D), lambda j: (0, 0))] * nx + [ANY] * len(after),
        out_specs=[o_spec] * len(types) + [pl.BlockSpec((m, D), lambda j: (0, 0))] * nx,
        out_shape=[jax.ShapeDtypeStruct((m, F), t) for t in types] + [jax.ShapeDtypeStruct((m, D), jnp.bfloat16)] * nx,
        scratch_shapes=[pltpu.VMEM((m, D), jnp.bfloat16)] if npc > 1 and not nx else [],
        compiler_params=_params(), cost_estimate=_cost(m, D, F * nw),
        name="up_dA" if slopes else "up_A",
    )(*pieces, *weights, *(slopes or ()), *([gamma[None]] if nx else []), *after)


def _down(parts, weights, dims, split=1, halves=(0, 1), after=(), tile=512):
    F = parts[0][0].shape[1]
    m, nb = sum(p.shape[0] for p in parts[0]), len(parts[0])
    ms = [p.shape[0] // split for p in parts[0] for _ in range(split)]
    nt = dims == NT
    D = weights[0].shape[0 if nt else 1]
    n = len(parts)
    half, nh = D // 2, len(halves)
    per = half // tile
    steps, off = nh * per, halves[0] * per
    nin = n * nb

    def body(*refs):
        ws, outs = refs[nin:nin + n], refs[nin + n + len(after):]
        cats = outs[nh * len(ms):] or [None] * n
        r = None
        for i in range(n):
            d = _dot(_fill(refs[i * nb:(i + 1) * nb], cats[i]), ws[i][...], dims)
            r = d if r is None else r + d

        for h in range(nh):
            @pl.when(pl.program_id(0) // per == h)
            def _():
                at = 0
                for b, rows in enumerate(ms):
                    outs[nh * b + h][...] = r[at:at + rows]
                    at += rows

    w_spec = pl.BlockSpec((tile, F), lambda j: (j + off, 0)) if nt else pl.BlockSpec((F, tile), lambda j: (0, j + off))
    places = [lambda j, h=h: (0, jnp.clip(j - h * per, 0, per - 1)) for h in range(nh)]
    blocks = [p for part in parts for p in part]
    out = pl.pallas_call(
        body, grid=(steps,),
        in_specs=[pl.BlockSpec(p.shape, lambda j: (0, 0)) for p in blocks] + [w_spec] * n + [ANY] * len(after),
        out_specs=[pl.BlockSpec((r, tile), f) for r in ms for f in places],
        out_shape=[jax.ShapeDtypeStruct((r, half), jnp.float32) for r in ms for _ in halves],
        scratch_shapes=[pltpu.VMEM((m, F), jnp.bfloat16)] * n if nb > 1 else [],
        compiler_params=_params(), cost_estimate=_cost(m, F * n, nh * half, 4 * m * nh * half),
        name="down",
    )(*blocks, *weights, *after)
    return [out[nh * b:nh * (b + 1)] for b in range(len(ms))]


def _grad(left, right, tile, after=()):
    m, N, M = sum(p.shape[0] for p in left), right[0].shape[1], left[0].shape[1]
    nl, nr = len(left), len(right)

    def body(*refs):
        ls, rs = refs[:nl], refs[nl:nl + nr]
        out, lcat, rcat = refs[-3:]
        at = 0
        for p in ls:
            lcat[at:at + p.shape[0]] = p[...]
            at += p.shape[0]
        _fill(rs, rcat)
        out[...] = _tn(lcat[...], rcat[...])

    return pl.pallas_call(
        body, grid=(M // tile,),
        in_specs=[pl.BlockSpec((p.shape[0], tile), lambda j: (0, j)) for p in left]
        + [pl.BlockSpec(p.shape, lambda j: (0, 0)) for p in right] + [ANY] * len(after),
        out_specs=pl.BlockSpec((tile, N), lambda j: (j, 0)),
        out_shape=jax.ShapeDtypeStruct((M, N), jnp.float32),
        scratch_shapes=[pltpu.VMEM((m, tile), jnp.bfloat16), pltpu.VMEM((m, N), jnp.bfloat16)],
        compiler_params=_params(), cost_estimate=_cost(M, m, N, 4 * M * N),
    )(*left, *right, *after)


def _finish(base, last, row, whole, n, tile, dgs=()):
    nw, ng = int(whole is not None), len(dgs)

    def body(*refs):
        gs, outs = refs[4:4 + ng], refs[4 + ng + nw:]
        half = outs[0].shape[1] // 2
        for h in range(2):
            outs[0][:, h * half:(h + 1) * half] = (refs[h][...] + refs[2 + h][...]).astype(outs[0].dtype)
        if ng:
            outs[1][...] = (gs[0][...] + gs[1][...]) + (gs[2][...] + gs[3][...])

    rows, half = last[0].shape
    at = lambda j: (j + row // tile, 0)
    spec = pl.BlockSpec((tile, half), at)
    one = pl.BlockSpec((1, 2 * half), lambda j: (0, 0))
    out = pl.pallas_call(
        body, grid=(rows // tile,),
        in_specs=[spec] * 2 + [pl.BlockSpec((tile, half), lambda j: (j, 0))] * 2 + [one] * ng + [ANY] * nw,
        out_specs=[pl.BlockSpec((tile, 2 * half), at)] + [one] * bool(ng),
        out_shape=[jax.ShapeDtypeStruct((n, 2 * half), jnp.bfloat16)] + [jax.ShapeDtypeStruct((1, 2 * half), jnp.float32)] * bool(ng),
        input_output_aliases={4 + ng: 0} if nw else {}, compiler_params=_params(),
        cost_estimate=pl.CostEstimate(flops=2 * rows * half, bytes_accessed=20 * rows * half, transcendentals=0),
        name="finish",
    )(*base, *last, *dgs, *([whole] if nw else []))
    return out if ng else out[0]


def _sums(pairs, pieces, tile):
    n, D = pairs[0][0].shape
    starts = [sum(pieces[:i]) // tile for i in range(len(pieces) + 1)]

    def body(*refs):
        ins, outs = refs[:2 * len(pairs)], refs[2 * len(pairs):]
        j = pl.program_id(0)
        for i in range(len(pairs)):
            r = ins[2 * i][...] + ins[2 * i + 1][...]
            for h in range(len(pieces)):
                @pl.when((j >= starts[h]) & (j < starts[h + 1]))
                def _():
                    outs[len(pieces) * i + h][...] = r

    spec = pl.BlockSpec((tile, D), lambda j: (j, 0))
    outs = [pl.BlockSpec((tile, D), lambda j, lo=lo, hi=hi: (jnp.clip(j - lo, 0, hi - lo - 1), 0))
            for lo, hi in zip(starts, starts[1:])]
    return pl.pallas_call(
        body, grid=(n // tile,), in_specs=[spec] * (2 * len(pairs)), out_specs=outs * len(pairs),
        out_shape=[jax.ShapeDtypeStruct((r, D), jnp.float32) for r in pieces] * len(pairs), compiler_params=_params(),
        cost_estimate=pl.CostEstimate(flops=2 * n * D, bytes_accessed=24 * n * D, transcendentals=0),
    )(*[v for p in pairs for v in p])


def _base(X, terms, tile=64):
    n, D = X.shape
    half = D // 2

    def body(x_ref, *refs):
        for h in range(2):
            x = x_ref[:, h * half:(h + 1) * half].astype(jnp.float32)
            refs[4 + h][...] = x + (refs[2 * h][...] + refs[2 * h + 1][...])

    spec = pl.BlockSpec((tile, half), lambda j: (j, 0))
    return pl.pallas_call(
        body, grid=(n // tile,), in_specs=[pl.BlockSpec((tile, D), lambda j: (j, 0))] + [spec] * 4, out_specs=[spec] * 2,
        out_shape=[jax.ShapeDtypeStruct((n, half), jnp.float32)] * 2, compiler_params=_params(),
        cost_estimate=pl.CostEstimate(flops=2 * n * D, bytes_accessed=14 * n * D, transcendentals=0), name="base",
    )(X, *[v for t in terms for v in t])


def _dx(terms, X, dY, gamma, tile=64):
    n, D = X.shape
    nt = len(terms[0])

    def body(x_ref, dy_ref, g_ref, *refs):
        ts, (out, dg) = refs[:2 * nt], refs[2 * nt:]
        halves = []
        for h in range(2):
            v = ts[h * nt][...]
            for t in ts[h * nt + 1:(h + 1) * nt]:
                v = v + t[...]
            halves.append(v)
        dXn = jnp.concatenate(halves, axis=1)
        xhatv, rstd = _ln(x_ref[...].astype(jnp.float32))
        part = jnp.sum(dXn * xhatv, axis=0, keepdims=True)

        @pl.when(pl.program_id(0) == 0)
        def _():
            dg[...] = part

        @pl.when(pl.program_id(0) > 0)
        def _():
            dg[...] += part

        dxhat = dXn * g_ref[...]
        dx = rstd * (dxhat - jnp.mean(dxhat, axis=-1, keepdims=True) - xhatv * jnp.mean(dxhat * xhatv, axis=-1, keepdims=True))
        out[...] = (dy_ref[...].astype(jnp.float32) + dx).astype(out.dtype)

    row = pl.BlockSpec((tile, D), lambda j: (j, 0))
    one = pl.BlockSpec((1, D), lambda j: (0, 0))
    return pl.pallas_call(
        body, grid=(n // tile,),
        in_specs=[row, row, one] + [pl.BlockSpec((tile, D // 2), lambda j: (j, 0))] * (2 * nt),
        out_specs=[row, one],
        out_shape=[jax.ShapeDtypeStruct((n, D), jnp.bfloat16), jax.ShapeDtypeStruct((1, D), jnp.float32)],
        compiler_params=_params(),
        cost_estimate=pl.CostEstimate(flops=20 * n * D, bytes_accessed=(6 + 4 * nt) * n * D, transcendentals=0),
        name="dx",
    )(X, dY, gamma[None], *terms[0], *terms[1])


def _halves(v):
    n, D = v.shape

    def body(ref, lo, hi):
        for h, out in enumerate((lo, hi)):
            @pl.when(pl.program_id(0) == h)
            def _():
                out[...] = ref[...]

    return pl.pallas_call(
        body, grid=(2,), in_specs=[pl.BlockSpec((n // 2, D), lambda j: (j, 0))],
        out_specs=[pl.BlockSpec((n // 2, D), lambda j: (0, 0))] * 2,
        out_shape=[jax.ShapeDtypeStruct((n // 2, D), v.dtype)] * 2, compiler_params=_params(),
        cost_estimate=pl.CostEstimate(flops=n * D, bytes_accessed=4 * n * D, transcendentals=0), name="halves",
    )(v)


def _tie(vals, after):
    return lax.optimization_barrier((tuple(vals), tuple(after)))[0]


def _near(v):
    return _cross(v, XN), _cross(v, YN)


def solution(mesh):
    rows = P(("data", "tp"), None)

    def block(X, gamma, W1, W2, dY):
        n, D = X.shape
        xx, xy = _near(X)
        W1p = _swap(W1, CORE)
        halves = _halves(dY)
        gx1, gy1 = _near(halves[0])
        gx2, gy2 = _near(halves[1])
        W2p = _swap(W2, CORE)
        Ws1, Ws2 = [W1, W1p], [W2, W2p]

        H0, s0, X0 = _up([X], [W1], NN, gamma=gamma)
        (A0,) = _up([dY], [W2], NT, slopes=(s0,))
        H0p, s0p, _ = _up([X], [W1p], NN, gamma=gamma, after=(A0,))
        xx, xy = _tie((xx, xy), (H0p,))
        xd = _cross(xx, YN)
        Hn, sn, Hnp, snp, Xn = _up([xx, xy], Ws1, NN, gamma=gamma, after=(H0p,))
        gx1, gy1 = _tie((gx1, gy1), (Hn,))
        gd1 = _cross(gy1, XN)
        (Yxa,), (Yya,) = _down([[Hn], [Hnp]], Ws2, NN, split=2, halves=(0,))
        gx2, gy2 = _tie((gx2, gy2), (Yxa,))
        gd2 = _cross(gy2, XN)
        (Yxb,), (Yyb,) = _down([[Hn], [Hnp]], Ws2, NN, split=2, halves=(1,), after=(Yxa,))
        Yx, Yy = (Yxa, Yxb), (Yya, Yyb)
        sa = _cross(Yx[0], XN)
        sb = _cross(Yy[1], YN)
        An, Anp = _up([gx1, gx2, gy1, gy2], Ws2, NT, slopes=(sn, snp), after=(Yxb,))
        Zx, Zy = _down([[An], [Anp]], Ws1, NT, split=2)
        ra = _cross(Zx[0], XN)
        rb = _cross(Zy[1], YN)
        Hd, sd, Hdp, sdp, Xd = _up([xd], Ws1, NN, gamma=gamma, after=(Zx[0],))
        Ad, Adp = _up([gd1, gd2], Ws2, NT, slopes=(sd, sdp))
        (Zd,) = _down([[Ad], [Adp]], Ws1, NT)
        fa = _cross(Zd[0], XN)
        fb = _cross(Zd[1], YN)
        (A0p,) = _up([dY], [W2p], NT, slopes=(s0p,), after=(Zd[0],))
        Y0, Yd = _down([[H0, Hd], [H0p, Hdp]], Ws2, NN, after=(A0p,))
        ya = _cross(Yd[0], XN)
        yb = _cross(Yd[1], YN)
        pair = lambda own, sent: own + [_swap(v, CORE) for v in _tie(sent, (Ad,))]
        dW1 = _grad(pair([X0, Xn, Xd], [X0, Xn, Xd]),
                      pair([A0, An, Ad], [A0p, Anp, Adp]), 512, after=(Yd[0],))
        Zx1, Zy0 = _tie((Zx[1], Zy[0]), (dW1,))
        far_a, far_b = _sums(((Zy0, fa), (Zx1, fb)), (n,), 64)
        za = _cross(far_a, YN)
        zb = _cross(far_b, XN)
        Gs = [dY, gx1, gx2, gy1, gy2, gd1, gd2]
        dW2 = _grad(pair([H0, Hn, Hd], [H0p, Hnp, Hdp]),
                      pair(Gs, Gs), 256, after=(far_a, far_b))
        Yx1, Yy0, Y00, Y01, X = _tie((Yx[1], Yy[0], Y0[0], Y0[1], X), (dW2,))
        cuts = n * 5 // 8, n // 4, n // 8
        sums = _sums(((Yy0, ya), (Yx1, yb)), cuts, n // 8)
        va, vb = _cross(sums[0], YN), _cross(sums[3], XN)
        ua, ub = _cross(sums[1], YN), _cross(sums[4], XN)
        base = _base(X, ((Y00, sa), (Y01, sb)))
        (Z0,) = _down([[A0], [A0p]], Ws1, NT, after=base)
        dX, dg = _dx(((Z0[0], ra, za), (Z0[1], rb, zb)), X, dY, gamma)
        dg = dg + _swap(dg, CORE)
        dgs = dg, _swap(dg, XN), _swap(dg, YN), _swap(dg, DIAG)
        last_a, last_b = _tie((sums[2], sums[5]), (dX,))
        wa = _cross(last_a, YN)
        wb = _cross(last_b, XN)
        Y = _finish(base, (va, vb), 0, None, n, cuts[0] // 2)
        Y = _finish(base, (ua, ub), cuts[0], Y, n, cuts[2])
        Y, dgamma = _finish(base, (wa, wb), cuts[0] + cuts[1], Y, n, cuts[2], dgs)
        return Y, dX, dW1, dW2, dgamma.reshape(D)

    return jax.shard_map(block, mesh=mesh,
                         in_specs=(rows, P(None), P(None, "tp"), P("tp", None), rows),
                         out_specs=(rows, rows, P("data", "tp"), rows, P("data")),
                         check_vma=False)
```

```python
import jax
import jax.numpy as jnp
from jax import lax
from jax.experimental import pallas as pl
from jax.experimental.pallas import tpu as pltpu
from jax.sharding import PartitionSpec as P


EPS = 1e-6


CORE, XN, YN, DIAG = 1, 2, 4, 6
NN = (((1,), (0,)), ((), ()))
NT = (((1,), (1,)), ((), ()))
ANY = pl.BlockSpec(memory_space=pl.ANY)


C1, C2 = 0.7978845608028654, 0.7978845608028654 * 0.044715


def _gelu(a):
    s = a * a
    q = 0.5 + 0.5 * jnp.tanh(a * (C1 + C2 * s))
    h = a * q
    return h, q + (h - h * q) * (2 * C1 + (6 * C2) * s)


def _ln(x):
    mu = jnp.mean(x, axis=-1, keepdims=True)
    xc = x - mu
    var = jnp.mean(xc * xc, axis=-1, keepdims=True)
    rstd = lax.rsqrt(var + EPS)
    return xc * rstd, rstd


def _tn(a, b):
    return lax.dot_general(a, b, (((0,), (0,)), ((), ())), preferred_element_type=jnp.float32)


def _dot(a, b, dims):
    return lax.dot_general(a, b, dims, preferred_element_type=jnp.float32)


def _swap(v, k):
    return lax.ppermute(v, "tp", [(i, i ^ k) for i in range(8)])


def _cross(v, k):
    return lax.ppermute(v, "tp", [(i, i ^ (k ^ DIAG if i % 2 else k)) for i in range(8)])


def _cost(m, k, n, extra=0):
    return pl.CostEstimate(flops=2 * m * k * n, bytes_accessed=2 * k * n + 2 * m * k + extra, transcendentals=0)


def _params():
    return pltpu.CompilerParams(dimension_semantics=("arbitrary",), vmem_limit_bytes=67_000_000)


def _fill(pieces, cat):
    if cat is None:
        return pieces[0][...]

    @pl.when(pl.program_id(0) == 0)
    def _():
        at = 0
        for p in pieces:
            cat[at:at + p.shape[0]] = p[...]
            at += p.shape[0]

    return cat[...]


def _norm(pieces, gamma, out, chunk=16):
    at = 0
    for p in pieces:
        def rows(i, _, p=p, at=at):
            r = pl.multiple_of(i * chunk, chunk)
            xhatv, _ = _ln(p[pl.ds(r, chunk)].astype(jnp.float32))
            out[pl.ds(at + r, chunk)] = (xhatv * gamma[...]).astype(out.dtype)
            return 0

        lax.fori_loop(0, p.shape[0] // chunk, rows, 0, unroll=4)
        at += p.shape[0]


def _up(pieces, weights, dims, slopes=None, gamma=None, after=(), tile=256):
    m, D = sum(p.shape[0] for p in pieces), pieces[0].shape[1]
    nt = dims == NT
    F = weights[0].shape[0 if nt else 1]
    nw, npc, ns, nx = len(weights), len(pieces), len(slopes or ()), int(gamma is not None)

    def body(*refs):
        ps, ws, ss = refs[:npc], refs[npc:npc + nw], refs[npc + nw:npc + nw + ns]
        outs = refs[npc + nw + ns + nx + len(after):]
        if nx:
            @pl.when(pl.program_id(0) == 0)
            def _():
                _norm(ps, refs[npc + nw + ns], outs[-1])

            a = outs[-1][...]
        else:
            a = _fill(ps, refs[-1] if npc > 1 else None)
        for i in range(nw):
            r = _dot(a, ws[i][...], dims)
            if slopes:
                outs[i][...] = (ss[i][...] * r).astype(jnp.bfloat16)
            else:
                h, slope = _gelu(r)
                outs[2 * i][...] = h.astype(jnp.bfloat16)
                outs[2 * i + 1][...] = slope

    w_spec = pl.BlockSpec((tile, D), lambda j: (j, 0)) if nt else pl.BlockSpec((D, tile), lambda j: (0, j))
    o_spec = pl.BlockSpec((m, tile), lambda j: (0, j))
    types = [jnp.bfloat16] * nw if slopes else [jnp.bfloat16, jnp.float32] * nw
    return pl.pallas_call(
        body, grid=(F // tile,),
        in_specs=[pl.BlockSpec(p.shape, lambda j: (0, 0)) for p in pieces] + [w_spec] * nw
        + [o_spec] * ns + [pl.BlockSpec((1, D), lambda j: (0, 0))] * nx + [ANY] * len(after),
        out_specs=[o_spec] * len(types) + [pl.BlockSpec((m, D), lambda j: (0, 0))] * nx,
        out_shape=[jax.ShapeDtypeStruct((m, F), t) for t in types] + [jax.ShapeDtypeStruct((m, D), jnp.bfloat16)] * nx,
        scratch_shapes=[pltpu.VMEM((m, D), jnp.bfloat16)] if npc > 1 and not nx else [],
        compiler_params=_params(), cost_estimate=_cost(m, D, F * nw),
        name="up_dA" if slopes else "up_A",
    )(*pieces, *weights, *(slopes or ()), *([gamma[None]] if nx else []), *after)


def _down(parts, weights, dims, split=1, halves=(0, 1), after=(), tile=512):
    F = parts[0][0].shape[1]
    m, nb = sum(p.shape[0] for p in parts[0]), len(parts[0])
    ms = [p.shape[0] // split for p in parts[0] for _ in range(split)]
    nt = dims == NT
    D = weights[0].shape[0 if nt else 1]
    n = len(parts)
    half, nh = D // 2, len(halves)
    per = half // tile
    steps, off = nh * per, halves[0] * per
    nin = n * nb

    def body(*refs):
        ws, outs = refs[nin:nin + n], refs[nin + n + len(after):]
        cats = outs[nh * len(ms):] or [None] * n
        r = None
        for i in range(n):
            d = _dot(_fill(refs[i * nb:(i + 1) * nb], cats[i]), ws[i][...], dims)
            r = d if r is None else r + d

        for h in range(nh):
            @pl.when(pl.program_id(0) // per == h)
            def _():
                at = 0
                for b, rows in enumerate(ms):
                    outs[nh * b + h][...] = r[at:at + rows]
                    at += rows

    w_spec = pl.BlockSpec((tile, F), lambda j: (j + off, 0)) if nt else pl.BlockSpec((F, tile), lambda j: (0, j + off))
    places = [lambda j, h=h: (0, jnp.clip(j - h * per, 0, per - 1)) for h in range(nh)]
    blocks = [p for part in parts for p in part]
    out = pl.pallas_call(
        body, grid=(steps,),
        in_specs=[pl.BlockSpec(p.shape, lambda j: (0, 0)) for p in blocks] + [w_spec] * n + [ANY] * len(after),
        out_specs=[pl.BlockSpec((r, tile), f) for r in ms for f in places],
        out_shape=[jax.ShapeDtypeStruct((r, half), jnp.float32) for r in ms for _ in halves],
        scratch_shapes=[pltpu.VMEM((m, F), jnp.bfloat16)] * n if nb > 1 else [],
        compiler_params=_params(), cost_estimate=_cost(m, F * n, nh * half, 4 * m * nh * half),
        name="down",
    )(*blocks, *weights, *after)
    return [out[nh * b:nh * (b + 1)] for b in range(len(ms))]


def _grad(left, right, tile, after=()):
    m, N, M = sum(p.shape[0] for p in left), right[0].shape[1], left[0].shape[1]
    nl, nr = len(left), len(right)

    def body(*refs):
        ls, rs = refs[:nl], refs[nl:nl + nr]
        out, lcat, rcat = refs[-3:]
        at = 0
        for p in ls:
            lcat[at:at + p.shape[0]] = p[...]
            at += p.shape[0]
        _fill(rs, rcat)
        out[...] = _tn(lcat[...], rcat[...])

    return pl.pallas_call(
        body, grid=(M // tile,),
        in_specs=[pl.BlockSpec((p.shape[0], tile), lambda j: (0, j)) for p in left]
        + [pl.BlockSpec(p.shape, lambda j: (0, 0)) for p in right] + [ANY] * len(after),
        out_specs=pl.BlockSpec((tile, N), lambda j: (j, 0)),
        out_shape=jax.ShapeDtypeStruct((M, N), jnp.float32),
        scratch_shapes=[pltpu.VMEM((m, tile), jnp.bfloat16), pltpu.VMEM((m, N), jnp.bfloat16)],
        compiler_params=_params(), cost_estimate=_cost(M, m, N, 4 * M * N),
    )(*left, *right, *after)


def _finish(base, last, row, whole, n, tile, dgs=()):
    nw, ng = int(whole is not None), len(dgs)

    def body(*refs):
        gs, outs = refs[3:3 + ng], refs[3 + ng + nw:]
        half = outs[0].shape[1] // 2
        for h in range(2):
            cols = slice(h * half, (h + 1) * half)
            outs[0][:, cols] = (refs[0][:, cols] + refs[1 + h][...]).astype(outs[0].dtype)
        if ng:
            outs[1][...] = (gs[0][...] + gs[1][...]) + (gs[2][...] + gs[3][...])

    rows, half = last[0].shape
    at = lambda j: (j + row // tile, 0)
    spec = pl.BlockSpec((tile, 2 * half), at)
    one = pl.BlockSpec((1, 2 * half), lambda j: (0, 0))
    out = pl.pallas_call(
        body, grid=(rows // tile,),
        in_specs=[spec] + [pl.BlockSpec((tile, half), lambda j: (j, 0))] * 2 + [one] * ng + [ANY] * nw,
        out_specs=[spec] + [one] * bool(ng),
        out_shape=[jax.ShapeDtypeStruct((n, 2 * half), jnp.bfloat16)] + [jax.ShapeDtypeStruct((1, 2 * half), jnp.float32)] * bool(ng),
        input_output_aliases={3 + ng: 0} if nw else {}, compiler_params=_params(),
        cost_estimate=pl.CostEstimate(flops=2 * rows * half, bytes_accessed=20 * rows * half, transcendentals=0),
        name="finish",
    )(base, *last, *dgs, *([whole] if nw else []))
    return out if ng else out[0]


def _sums(pairs, pieces, tile):
    n, D = pairs[0][0].shape
    starts = [sum(pieces[:i]) // tile for i in range(len(pieces) + 1)]

    def body(*refs):
        ins, outs = refs[:2 * len(pairs)], refs[2 * len(pairs):]
        j = pl.program_id(0)
        for i in range(len(pairs)):
            r = ins[2 * i][...] + ins[2 * i + 1][...]
            for h in range(len(pieces)):
                @pl.when((j >= starts[h]) & (j < starts[h + 1]))
                def _():
                    outs[len(pieces) * i + h][...] = r

    spec = pl.BlockSpec((tile, D), lambda j: (j, 0))
    outs = [pl.BlockSpec((tile, D), lambda j, lo=lo, hi=hi: (jnp.clip(j - lo, 0, hi - lo - 1), 0))
            for lo, hi in zip(starts, starts[1:])]
    return pl.pallas_call(
        body, grid=(n // tile,), in_specs=[spec] * (2 * len(pairs)), out_specs=outs * len(pairs),
        out_shape=[jax.ShapeDtypeStruct((r, D), jnp.float32) for r in pieces] * len(pairs), compiler_params=_params(),
        cost_estimate=pl.CostEstimate(flops=2 * n * D, bytes_accessed=24 * n * D, transcendentals=0),
    )(*[v for p in pairs for v in p])


def _base(X, terms, tile=64):
    n, D = X.shape
    half = D // 2

    def body(x_ref, *refs):
        for h in range(2):
            x = x_ref[:, h * half:(h + 1) * half].astype(jnp.float32)
            refs[4][:, h * half:(h + 1) * half] = x + (refs[2 * h][...] + refs[2 * h + 1][...])

    spec = pl.BlockSpec((tile, half), lambda j: (j, 0))
    return pl.pallas_call(
        body, grid=(n // tile,), in_specs=[pl.BlockSpec((tile, D), lambda j: (j, 0))] + [spec] * 4,
        out_specs=pl.BlockSpec((tile, D), lambda j: (j, 0)),
        out_shape=jax.ShapeDtypeStruct((n, D), jnp.float32), compiler_params=_params(),
        cost_estimate=pl.CostEstimate(flops=2 * n * D, bytes_accessed=14 * n * D, transcendentals=0), name="base",
    )(X, *[v for t in terms for v in t])


def _dx(terms, X, dY, gamma, tile=64):
    n, D = X.shape
    nt = len(terms[0])

    def body(x_ref, dy_ref, g_ref, *refs):
        ts, (out, dg) = refs[:2 * nt], refs[2 * nt:]
        halves = []
        for h in range(2):
            v = ts[h * nt][...]
            for t in ts[h * nt + 1:(h + 1) * nt]:
                v = v + t[...]
            halves.append(v)
        dXn = jnp.concatenate(halves, axis=1)
        xhatv, rstd = _ln(x_ref[...].astype(jnp.float32))
        part = jnp.sum(dXn * xhatv, axis=0, keepdims=True)

        @pl.when(pl.program_id(0) == 0)
        def _():
            dg[...] = part

        @pl.when(pl.program_id(0) > 0)
        def _():
            dg[...] += part

        dxhat = dXn * g_ref[...]
        dx = rstd * (dxhat - jnp.mean(dxhat, axis=-1, keepdims=True) - xhatv * jnp.mean(dxhat * xhatv, axis=-1, keepdims=True))
        out[...] = (dy_ref[...].astype(jnp.float32) + dx).astype(out.dtype)

    row = pl.BlockSpec((tile, D), lambda j: (j, 0))
    one = pl.BlockSpec((1, D), lambda j: (0, 0))
    return pl.pallas_call(
        body, grid=(n // tile,),
        in_specs=[row, row, one] + [pl.BlockSpec((tile, D // 2), lambda j: (j, 0))] * (2 * nt),
        out_specs=[row, one],
        out_shape=[jax.ShapeDtypeStruct((n, D), jnp.bfloat16), jax.ShapeDtypeStruct((1, D), jnp.float32)],
        compiler_params=_params(),
        cost_estimate=pl.CostEstimate(flops=20 * n * D, bytes_accessed=(6 + 4 * nt) * n * D, transcendentals=0),
        name="dx",
    )(X, dY, gamma[None], *terms[0], *terms[1])


def _halves(v):
    n, D = v.shape

    def body(ref, lo, hi):
        for h, out in enumerate((lo, hi)):
            @pl.when(pl.program_id(0) == h)
            def _():
                out[...] = ref[...]

    return pl.pallas_call(
        body, grid=(2,), in_specs=[pl.BlockSpec((n // 2, D), lambda j: (j, 0))],
        out_specs=[pl.BlockSpec((n // 2, D), lambda j: (0, 0))] * 2,
        out_shape=[jax.ShapeDtypeStruct((n // 2, D), v.dtype)] * 2, compiler_params=_params(),
        cost_estimate=pl.CostEstimate(flops=n * D, bytes_accessed=4 * n * D, transcendentals=0), name="halves",
    )(v)


def _tie(vals, after):
    return lax.optimization_barrier((tuple(vals), tuple(after)))[0]


def _near(v):
    return _cross(v, XN), _cross(v, YN)


def solution(mesh):
    rows = P(("data", "tp"), None)

    def block(X, gamma, W1, W2, dY):
        n, D = X.shape
        xx, xy = _near(X)
        W1p = _swap(W1, CORE)
        halves = _halves(dY)
        gx1, gy1 = _near(halves[0])
        gx2, gy2 = _near(halves[1])
        W2p = _swap(W2, CORE)
        Ws1, Ws2 = [W1, W1p], [W2, W2p]

        H0, s0, X0 = _up([X], [W1], NN, gamma=gamma)
        (A0,) = _up([dY], [W2], NT, slopes=(s0,))
        H0p, s0p, _ = _up([X], [W1p], NN, gamma=gamma, after=(A0,))
        xx, xy = _tie((xx, xy), (H0p,))
        xd = _cross(xx, YN)
        Hn, sn, Hnp, snp, Xn = _up([xx, xy], Ws1, NN, gamma=gamma, after=(H0p,))
        gx1, gy1 = _tie((gx1, gy1), (Hn,))
        gd1 = _cross(gy1, XN)
        (Yxa,), (Yya,) = _down([[Hn], [Hnp]], Ws2, NN, split=2, halves=(0,))
        gx2, gy2 = _tie((gx2, gy2), (Yxa,))
        gd2 = _cross(gy2, XN)
        (Yxb,), (Yyb,) = _down([[Hn], [Hnp]], Ws2, NN, split=2, halves=(1,), after=(Yxa,))
        Yx, Yy = (Yxa, Yxb), (Yya, Yyb)
        sa = _cross(Yx[0], XN)
        sb = _cross(Yy[1], YN)
        An, Anp = _up([gx1, gx2, gy1, gy2], Ws2, NT, slopes=(sn, snp), after=(Yxb,))
        Zx, Zy = _down([[An], [Anp]], Ws1, NT, split=2)
        ra = _cross(Zx[0], XN)
        rb = _cross(Zy[1], YN)
        Hd, sd, Hdp, sdp, Xd = _up([xd], Ws1, NN, gamma=gamma, after=(Zx[0],))
        Ad, Adp = _up([gd1, gd2], Ws2, NT, slopes=(sd, sdp))
        (Zd,) = _down([[Ad], [Adp]], Ws1, NT)
        fa = _cross(Zd[0], XN)
        fb = _cross(Zd[1], YN)
        (A0p,) = _up([dY], [W2p], NT, slopes=(s0p,), after=(Zd[0],))
        Y0, Yd = _down([[H0, Hd], [H0p, Hdp]], Ws2, NN, after=(A0p,))
        ya = _cross(Yd[0], XN)
        yb = _cross(Yd[1], YN)
        pair = lambda own, sent: own + [_swap(v, CORE) for v in _tie(sent, (Ad,))]
        dW1 = _grad(pair([X0, Xn, Xd], [X0, Xn, Xd]),
                      pair([A0, An, Ad], [A0p, Anp, Adp]), 512, after=(Yd[0],))
        Zx1, Zy0 = _tie((Zx[1], Zy[0]), (dW1,))
        far_a, far_b = _sums(((Zy0, fa), (Zx1, fb)), (n,), 64)
        za = _cross(far_a, YN)
        zb = _cross(far_b, XN)
        Gs = [dY, gx1, gx2, gy1, gy2, gd1, gd2]
        dW2 = _grad(pair([H0, Hn, Hd], [H0p, Hnp, Hdp]),
                      pair(Gs, Gs), 256, after=(far_a, far_b))
        Yx1, Yy0, Y00, Y01, X = _tie((Yx[1], Yy[0], Y0[0], Y0[1], X), (dW2,))
        cuts = n * 5 // 8, n // 4, n // 8
        sums = _sums(((Yy0, ya), (Yx1, yb)), cuts, n // 8)
        va, vb = _cross(sums[0], YN), _cross(sums[3], XN)
        ua, ub = _cross(sums[1], YN), _cross(sums[4], XN)
        base = _base(X, ((Y00, sa), (Y01, sb)))
        (Z0,) = _down([[A0], [A0p]], Ws1, NT, after=(base,))
        dX, dg = _dx(((Z0[0], ra, za), (Z0[1], rb, zb)), X, dY, gamma)
        dg = dg + _swap(dg, CORE)
        dgs = dg, _swap(dg, XN), _swap(dg, YN), _swap(dg, DIAG)
        last_a, last_b = _tie((sums[2], sums[5]), (dX,))
        wa = _cross(last_a, YN)
        wb = _cross(last_b, XN)
        Y = _finish(base, (va, vb), 0, None, n, cuts[0] // 2)
        Y = _finish(base, (ua, ub), cuts[0], Y, n, cuts[2])
        Y, dgamma = _finish(base, (wa, wb), cuts[0] + cuts[1], Y, n, cuts[2] // 2, dgs)
        return Y, dX, dW1, dW2, dgamma.reshape(D)

    return jax.shard_map(block, mesh=mesh,
                         in_specs=(rows, P(None), P(None, "tp"), P("tp", None), rows),
                         out_specs=(rows, rows, P("data", "tp"), rows, P("data")),
                         check_vma=False)
```
